32 devices in a mesh: wide: 4 (over y, x), grp: 8 (over z, core).
Axes of the slice: x: 2, y: 2, z: 4, core: 2. Of those that a mesh axis runs over, the one named last changes fastest.
Arguments:
- surf_depth: int32 [4, 8, 8, 4096], P('wide', 'grp'), may hold values from 0 to 1073741823
- surf_color: bfloat16 [4, 8, 8, 3, 4096], P('wide', 'grp'), may hold values from 0 to 2
- surf_box: int32 [4, 8, 8, 4], P('wide', 'grp'), may hold values from 0 to 64, as said below
- vol_color: bfloat16 [4, 8, 4, 8, 3, 4096], P('wide', 'grp'), may hold values from 0 to 4
- vol_alpha: bfloat16 [4, 8, 4, 8, 4096], P('wide', 'grp'), may hold values from 0.0009994507 to 0.039794922
- vol_box: int32 [4, 8, 4, 4], P('wide', 'grp'), may hold values from 0 to 64, as said below
- ray_entry: int32 [4, 8, 4, 4096], P('wide', 'grp'), may hold values from 0 to 939524095
- ray_step: int32 [4, 8, 4, 4096], P('wide', 'grp'), may hold values from 1048576 to 16777215
- order: int32 [8, 4], P('grp'), may hold values from 0 to 3, each once within a row
Outputs:
- frame: float32 [8, 4, 4, 4096], P('grp', 'wide')
The draws below stay inside these ranges and needn't reach their ends.
Inputs may be any that keep to these rules, and one draw needn't show every extreme that they name: `surf_box`: each box gives rows [top, bottom) and columns [left, right) of a tile with 1 to 16 rows and 1 or more columns; in every draw one tile row has boxes of exactly 16 rows from every source, and other tiles reach it too. `vol_box`: each box gives rows [top, bottom) and columns [left, right) of a tile with 1 to 32 rows and 1 or more columns; in every draw one tile column has boxes of exactly 32 rows from every brick of every band, and other tiles reach it too. `order`: each row is a permutation of 0 .. 3.
All inputs are finite; a program needn't handle non-finite values.
Results may differ from the reference program's by a relative error of at most 0.0003.
Values may be sent and summed in bfloat16 or wider, within the bound.
A program may use at most 64 MiB of HBM per device.

```python
import math
import jax
import jax.numpy as jnp
from jax import lax

TILE_H = 64
TILE_W = 64
TPIX = 4096
SAMPLES = 8
SBOX_ROWS = 16
VBOX_ROWS = 32
N_WIDE = 4
N_GRP = 8


def draw_boxes(key, lead, most, full_axis):
    keys = jax.random.split(key, 6)
    height = jax.random.randint(keys[0], lead, 1, most + 1)
    force = jax.random.randint(keys[1], lead, 0, 4) == 0
    chosen = jax.random.randint(keys[2], (), 0, lead[full_axis])
    position = lax.broadcasted_iota(jnp.int32, lead, full_axis)
    height = jnp.where(force | (position == chosen), most, height)
    top = jax.random.randint(keys[3], lead, 0, TILE_H - height + 1)
    width = jax.random.randint(keys[4], lead, 1, TILE_W + 1)
    left = jax.random.randint(keys[5], lead, 0, TILE_W - width + 1)
    return jnp.stack([top, top + height, left, left + width], axis=-1).astype(jnp.int32)


def draw_surf_box(key, part):
    return draw_boxes(jax.random.fold_in(key, 11), (N_WIDE, N_GRP, N_GRP), SBOX_ROWS, 2)


def draw_vol_box(key, part):
    return draw_boxes(jax.random.fold_in(key, 23), (N_WIDE, N_GRP, N_WIDE), VBOX_ROWS, 2)


def plant(entries, rng, smallest, largest):
    extent = entries.shape
    spot = [jax.random.randint(jax.random.fold_in(rng, axis), (), 0, extent[axis]) for axis in range(len(extent))]
    entries = entries.at[tuple(spot)].set(smallest)
    longest = extent.index(max(extent))
    spot[longest] = (spot[longest] + 1) % extent[longest]
    return entries.at[tuple(spot)].set(largest)


def levels(own_key, extent, pieces, smallest, high):
    factor_of = 1.0
    for dim, shards_of in pieces:
        steps = jax.random.uniform(jax.random.fold_in(jax.random.fold_in(own_key, 6), dim), (shards_of,), jnp.float32, smallest / len(pieces), high / len(pieces))
        factor_of = factor_of * jnp.repeat(jnp.exp(steps), extent[dim] // shards_of).reshape((-1,) + (1,) * (len(extent) - 1 - dim))
    return factor_of


def setup_inputs(seed: int = 0) -> dict:
    arg_keys = jax.random.split(jax.random.key(seed), 10)
    surf_depth = plant(jax.random.randint(arg_keys[0], (N_WIDE, N_GRP, N_GRP, TPIX), 0, 1073741824), jax.random.fold_in(arg_keys[0], 1), 0, 1073741823).astype(jnp.int32)
    surf_color = jnp.clip(2.0 * jax.random.uniform(arg_keys[1], (N_WIDE, N_GRP, N_GRP, 3, TPIX), jnp.float32) ** levels(arg_keys[1], (N_WIDE, N_GRP, N_GRP, 3, TPIX), ((0, 4), (1, 8)), -0.2, 0.2), 0.0, 2.0).astype(jnp.bfloat16)
    surf_box = draw_surf_box(jax.random.fold_in(arg_keys[9], 71), 0)
    vol_color = jnp.clip(4.0 * jax.random.uniform(arg_keys[3], (N_WIDE, N_GRP, N_WIDE, SAMPLES, 3, TPIX), jnp.float32) ** levels(arg_keys[3], (N_WIDE, N_GRP, N_WIDE, SAMPLES, 3, TPIX), ((0, 4), (1, 8)), -0.2, 0.2), 0.0, 4.0).astype(jnp.bfloat16)
    vol_alpha = jnp.clip(jnp.exp(math.log(0.039794922) - 3.6842888 * jax.random.uniform(arg_keys[4], (N_WIDE, N_GRP, N_WIDE, SAMPLES, TPIX), jnp.float32) ** levels(arg_keys[4], (N_WIDE, N_GRP, N_WIDE, SAMPLES, TPIX), ((0, 4), (1, 8)), -0.2, 0.2)), 0.0009994507, 0.039794922).astype(jnp.bfloat16)
    vol_box = draw_vol_box(jax.random.fold_in(arg_keys[9], 71), 0)
    ray_entry = plant(jax.random.randint(arg_keys[6], (N_WIDE, N_GRP, N_WIDE, TPIX), 0, 939524096), jax.random.fold_in(arg_keys[6], 1), 0, 939524095).astype(jnp.int32)
    ray_step = plant(jax.random.randint(arg_keys[7], (N_WIDE, N_GRP, N_WIDE, TPIX), 1048576, 16777216), jax.random.fold_in(arg_keys[7], 1), 1048576, 16777215).astype(jnp.int32)
    order = jax.vmap(lambda own: jax.random.permutation(own, N_WIDE))(jax.random.split(arg_keys[8], N_GRP)).reshape((N_GRP, N_WIDE)).astype(jnp.int32)
    return dict(surf_depth=surf_depth, surf_color=surf_color, surf_box=surf_box, vol_color=vol_color, vol_alpha=vol_alpha, vol_box=vol_box, ray_entry=ray_entry, ray_step=ray_step, order=order)


far_depth = 1073741824


def window_mask(box, start, rows, tile_w):
    row_ids = start[..., None, None] + jnp.arange(rows, dtype=jnp.int32)[:, None]
    col_ids = jnp.arange(tile_w, dtype=jnp.int32)[None, :]
    inside = (row_ids >= box[..., 0, None, None]) & (row_ids < box[..., 1, None, None])
    inside = inside & (col_ids >= box[..., 2, None, None]) & (col_ids < box[..., 3, None, None])
    return inside.reshape(box.shape[:-1] + (rows * tile_w,))


def integrate(color, alpha, inside, entry, stride, limit):
    accum = jnp.zeros(alpha.shape[:-2] + (3, alpha.shape[-1]), jnp.float32)
    trans = jnp.ones(alpha.shape[:-2] + (alpha.shape[-1],), jnp.float32)
    for k in range(SAMPLES):
        kept = inside & (entry + k * stride < limit)
        opacity = alpha[..., k, :].astype(jnp.float32)
        weight = jnp.where(kept, trans * opacity, 0.0)
        accum = accum + weight[..., None, :] * color[..., k, :, :].astype(jnp.float32)
        trans = trans * (1.0 - jnp.where(kept, opacity, 0.0))
    return accum, trans


def reference(surf_depth, surf_color, surf_box, vol_color, vol_alpha, vol_box, ray_entry, ray_step, order):
    present = window_mask(surf_box, jnp.zeros(surf_box.shape[:-1], jnp.int32), TILE_H, TILE_W)
    frag_depth = jnp.where(present, surf_depth, far_depth)
    nearest = jnp.min(frag_depth, axis=1)
    winner = jnp.argmin(frag_depth, axis=1).astype(jnp.int32)
    sources = jnp.arange(N_GRP, dtype=jnp.int32)[None, :, None, None]
    pick = (sources == winner[:, None]) & present
    surface = jnp.sum(jnp.where(pick[:, :, :, None, :], surf_color.astype(jnp.float32), 0.0), axis=1)

    def one_band(band):
        color = lax.dynamic_index_in_dim(vol_color, band, 1, keepdims=False)
        alpha = lax.dynamic_index_in_dim(vol_alpha, band, 1, keepdims=False)
        box = lax.dynamic_index_in_dim(vol_box, band, 1, keepdims=False)
        entry = lax.dynamic_index_in_dim(ray_entry, band, 1, keepdims=False)
        stride = lax.dynamic_index_in_dim(ray_step, band, 1, keepdims=False)
        limit = lax.dynamic_index_in_dim(nearest, band, 1, keepdims=False)
        inside = window_mask(box, jnp.zeros(box.shape[:-1], jnp.int32), TILE_H, TILE_W)
        accum, trans = integrate(color, alpha, inside, entry, stride, limit[None])
        rank = lax.dynamic_index_in_dim(order, band, 0, keepdims=False)
        ordered_accum = jnp.take(accum, rank, axis=0)
        ordered_trans = jnp.take(trans, rank, axis=0)

        def over(carry, layer):
            color_sum, through = carry
            return (color_sum + through[:, None, :] * layer[0], through * layer[1]), None

        start = (jnp.zeros(accum.shape[1:], jnp.float32), jnp.ones(trans.shape[1:], jnp.float32))
        (color_sum, through), unused = lax.scan(over, start, (ordered_accum, ordered_trans))
        behind = lax.dynamic_index_in_dim(surface, band, 1, keepdims=False)
        rgb = color_sum + through[:, None, :] * behind
        return jnp.concatenate([rgb, through[:, None, :]], axis=1)

    return lax.map(one_band, jnp.arange(N_GRP, dtype=jnp.int32))
```

```python
import functools

import jax
import jax.numpy as jnp
from jax import lax
from jax.experimental import pallas as pl
from jax.experimental.pallas import tpu as pltpu
from jax.sharding import PartitionSpec as P

TILE_H = 64
TILE_W = 64
SBOX_ROWS = 16
VBOX_ROWS = 32
LANES = 128

far_depth = 1073741824
MESH_ID = pl.DeviceIdType.MESH

NG = TILE_H * TILE_W // LANES
SG = SBOX_ROWS * TILE_W // LANES + 1
VG = VBOX_ROWS * TILE_W // LANES + 1
SPAD = NG - SG
VPAD = NG - VG


def group_of(top, pad):
    return jnp.minimum(lax.div(top * TILE_W, LANES), pad)


def window_inside(box, row, group, groups):
    top, bottom, left, right = [box(row, i) for i in range(4)]
    shape = (groups, 1, LANES)
    lane = lax.broadcasted_iota(jnp.int32, shape, 2)
    pix = lane + (lax.broadcasted_iota(jnp.int32, shape, 0) + group) * LANES
    col = lane & (TILE_W - 1)
    inside = (pix >= top * TILE_W) & (pix < bottom * TILE_W)
    return inside & (col >= left) & (col < right)


def groups_of(load, start, count):
    return jnp.stack([load(start + j) for j in range(count)])


def kernel(
    nw, ng, sbox_t, vbox, order, sbox_v, vbox_v, sdepth, scolor, vcolor, valpha, rentry, rstep,
    out,
    depth_in, scolor_in, color_in, alpha_in, entry_in, step_in,
    sbox_r, vbox_r, sbox_m, vbox_m, dsend, drecv, csend, crecv, winner, surface, vsend, vrecv,
    load_sem, sb_s, sb_r, vb_s, vb_r, d_s, d_r, c_s, c_r, l_s, l_r, v_s, v_r, *limits,
):
    w = lax.axis_index("wide")
    g = lax.axis_index("grp")
    samples = alpha_in.shape[2]

    def sbox(r, i):
        return sbox_t[i, r]

    def vbox_at(c, i):
        return vbox[c, i]

    loads = [
        pltpu.make_async_copy(src, dst, load_sem.at[i])
        for i, (src, dst) in enumerate(
            [(sdepth, depth_in), (scolor, scolor_in), (valpha, alpha_in), (rentry, entry_in), (rstep, step_in), (vcolor, color_in)]
        )
    ]
    loads[0].start()

    barrier = pltpu.get_barrier_semaphore()
    for i in range(1, ng):
        pl.semaphore_signal(barrier, inc=1, device_id=(w, lax.rem(g + i, ng)), device_id_type=MESH_ID)
    for i in range(1, nw):
        pl.semaphore_signal(barrier, inc=1, device_id=(lax.rem(w + i, nw), g), device_id_type=MESH_ID)
    for copy in loads[1:]:
        copy.start()

    loads[0].wait()
    for r in range(ng):
        start = group_of(sbox(r, 0), SPAD)
        inside = window_inside(sbox, r, start, SG)
        depth = groups_of(lambda j: depth_in[j, r : r + 1], start, SG)
        dsend[r] = jnp.where(inside, depth, far_depth)

    pl.semaphore_wait(barrier, ng - 1 + nw - 1)

    def remote(src, dst, send, recv, device):
        return pltpu.make_async_remote_copy(
            src_ref=src, dst_ref=dst, send_sem=send, recv_sem=recv, device_id=device, device_id_type=MESH_ID
        )

    sends = []
    dcopies, ccopies, scopies, vbcopies = [], [], [], []
    for i in range(1, ng):
        peer = lax.rem(g + i, ng)
        scopies.append(remote(sbox_v, sbox_r.at[g], sb_s.at[i], sb_r.at[i], (w, peer)))
        scopies[-1].start()
        dcopies.append(
            remote(
                dsend.at[peer], drecv.at[g, pl.ds(SPAD, SG)], d_s.at[i], d_r.at[i], (w, peer)
            )
        )
        dcopies[-1].start()
    for i in range(1, nw):
        peer = lax.rem(w + i, nw)
        vbcopies.append(remote(vbox_v, vbox_r.at[w], vb_s.at[i], vb_r.at[i], (peer, g)))
        vbcopies[-1].start()
    loads[1].wait()
    for r in range(ng):
        start = group_of(sbox(r, 0), SPAD)
        for ch in range(3):
            color = groups_of(lambda j: scolor_in[ch, j].astype(jnp.float32)[r : r + 1], start, SG)
            csend[r, :, ch : ch + 1] = color
    middle = pl.ds(SPAD, SG)
    for i in range(1, ng):
        peer = lax.rem(g + i, ng)
        ccopies.append(remote(csend.at[peer], crecv.at[g, middle], c_s.at[i], c_r.at[i], (w, peer)))
        ccopies[-1].start()
    crecv[g, middle] = csend[g]

    sbox_r[g] = sbox_v[...]
    vbox_r[w] = vbox_v[...]
    drecv[g, middle] = dsend[g]
    for s in range(ng):
        drecv[s, :SPAD] = jnp.full((SPAD, 1, LANES), far_depth, jnp.int32)
        drecv[s, SPAD + SG :] = jnp.full((SPAD, 1, LANES), far_depth, jnp.int32)
    pad_row = lax.broadcasted_iota(jnp.int32, (VPAD, 4, LANES), 1)
    pad = jnp.where(pad_row == 3, 1.0, 0.0)
    for b in range(nw):
        vrecv[b, :VPAD] = pad
        vrecv[b, VPAD + VG :] = pad

    for copy in scopies:
        copy.wait_recv()
    to_smem = pltpu.make_async_copy(sbox_r, sbox_m, load_sem.at[6])
    to_smem.start()
    to_smem.wait()
    starts = [SPAD - group_of(sbox_m[s, 0, g], SPAD) for s in range(ng)]
    for copy in dcopies:
        copy.wait_recv()
    step = NG // 4

    for q in range(4):
        best = groups_of(lambda j: drecv[0, j], starts[0] + q * step, step)
        win = jnp.zeros_like(best)
        for s in range(1, ng):
            depth = groups_of(lambda j: drecv[s, j], starts[s] + q * step, step)
            win = jnp.where(depth < best, s, win)
            best = jnp.minimum(depth, best)
        limits[0][q * step : (q + 1) * step] = best
        winner[q * step : (q + 1) * step] = jnp.where(best < far_depth, win, -1)

    lcopies = []
    for i in range(1, nw):
        lcopies.append(remote(limits[0], limits[i], l_s.at[i], l_r.at[i], (lax.rem(w + i, nw), g)))
        lcopies[-1].start()
    for copy in loads[2:]:
        copy.wait()

    k_ids = lax.broadcasted_iota(jnp.int32, (VG, samples, LANES), 1)

    def integrate(c, limit):
        start = group_of(vbox[c, 0], VPAD)
        inside = window_inside(vbox_at, c, start, VG)
        bound = jnp.where(inside, groups_of(lambda j: limit[j], start, VG), -1)
        entry = groups_of(lambda j: entry_in[j, pl.ds(c, 1)], start, VG)
        stride = groups_of(lambda j: step_in[j, pl.ds(c, 1)], start, VG)
        kept = entry + k_ids * stride < bound
        alpha = groups_of(lambda j: alpha_in[c, j].astype(jnp.float32), start, VG)
        opacity = jnp.where(kept, alpha, 0.0)
        clear = 1.0 - opacity
        before = jnp.where(k_ids >= 1, pltpu.roll(clear, 1, 1), 1.0)
        shift = 1
        while shift < samples:
            before = before * jnp.where(k_ids >= shift, pltpu.roll(before, shift, 1), 1.0)
            shift *= 2
        weight = opacity * before
        accum = []
        for ch in range(3):
            color = groups_of(lambda j: color_in[c, ch, j].astype(jnp.float32), start, VG)
            accum.append(jnp.sum(weight * color, axis=1, keepdims=True))
        return accum, (before * clear)[:, samples - 1 : samples]

    accum, trans = integrate(w, limits[0])
    window = pl.ds(VPAD, VG)
    for ch in range(3):
        vrecv[w, window, ch : ch + 1] = accum[ch]
    vrecv[w, window, 3:4] = trans

    def vcopy(i):
        c = lax.rem(w + nw - i, nw)
        return remote(vsend.at[c], vrecv.at[w, window], v_s.at[i], v_r.at[i], (c, g))

    for i in range(1, nw):
        c = lax.rem(w + nw - i, nw)
        lcopies[i - 1].wait_recv()
        accum, trans = integrate(c, limits[i])
        for ch in range(3):
            vsend[c, :, ch : ch + 1] = accum[ch]
        vsend[c, :, 3:4] = trans
        vcopy(i).start()

    for copy in ccopies:
        copy.wait_recv()
    for q in range(4):
        win = winner[q * step : (q + 1) * step]
        color = jnp.zeros((step, 3, LANES), jnp.float32)
        for s in range(ng):
            color = jnp.where(win == s, groups_of(lambda j: crecv[s, j], starts[s] + q * step, step), color)
        surface[q * step : (q + 1) * step] = color

    for copy in vbcopies:
        copy.wait_recv()
    to_smem = pltpu.make_async_copy(vbox_r, vbox_m, load_sem.at[7])
    to_smem.start()
    to_smem.wait()
    ranks = [order[0, j] for j in range(nw)]
    offsets = [VPAD - group_of(vbox_m[b, w, 0], VPAD) for b in ranks]
    for i in range(1, nw):
        vcopy(i).wait_recv()
    for q in range(4):
        color = jnp.zeros((step, 3, LANES), jnp.float32)
        through = jnp.ones((step, 1, LANES), jnp.float32)
        for j in range(nw):
            layer = groups_of(lambda i: vrecv[ranks[j], i], offsets[j] + q * step, step)
            color = color + through * layer[:, 0:3]
            through = through * layer[:, 3:4]
        color = color + through * surface[q * step : (q + 1) * step]
        for j in range(step):
            at = slice((q * step + j) * LANES, (q * step + j + 1) * LANES)
            out[0:3, at] = color[j]
            out[3:4, at] = through[j]

    for copy in scopies + dcopies + vbcopies + ccopies + lcopies:
        copy.wait_send()
    for i in range(1, nw):
        vcopy(i).wait_send()


def solution(mesh):
    nw, ng = mesh.shape["wide"], mesh.shape["grp"]

    def per_device(sdepth, scolor, sbox, vcolor, valpha, vbox, rentry, rstep, order):
        sdepth, scolor, sbox = sdepth[0, 0], scolor[0, 0].transpose(1, 0, 2), sbox[0, 0].T
        vcolor, valpha, vbox = vcolor[0, 0].transpose(0, 2, 1, 3), valpha[0, 0], vbox[0, 0]
        rentry, rstep = rentry[0, 0], rstep[0, 0]
        pix = TILE_H * TILE_W

        def grouped(x):
            x = x.reshape(x.shape[:-1] + (NG, LANES))
            return jnp.moveaxis(x, -2, -3)

        sdepth, scolor, vcolor, valpha = grouped(sdepth), grouped(scolor), grouped(vcolor), grouped(valpha)
        rentry, rstep = grouped(rentry), grouped(rstep)
        smem = pl.BlockSpec(memory_space=pltpu.SMEM)
        vmem = pl.BlockSpec(memory_space=pltpu.VMEM)
        hbm = pl.BlockSpec(memory_space=pl.ANY)
        dma = pltpu.SemaphoreType.DMA
        frame = pl.pallas_call(
            functools.partial(kernel, nw, ng),
            out_shape=jax.ShapeDtypeStruct((4, pix), jnp.float32),
            in_specs=[smem] * 3 + [vmem] * 2 + [hbm] * 6,
            out_specs=vmem,
            scratch_shapes=[
                pltpu.VMEM(sdepth.shape, jnp.int32),
                pltpu.VMEM(scolor.shape, jnp.bfloat16),
                pltpu.VMEM(vcolor.shape, jnp.bfloat16),
                pltpu.VMEM(valpha.shape, jnp.bfloat16),
                pltpu.VMEM(rentry.shape, jnp.int32),
                pltpu.VMEM(rstep.shape, jnp.int32),
                pltpu.VMEM((ng,) + sbox.shape, jnp.int32),
                pltpu.VMEM((nw,) + vbox.shape, jnp.int32),
                pltpu.SMEM((ng,) + sbox.shape, jnp.int32),
                pltpu.SMEM((nw,) + vbox.shape, jnp.int32),
                pltpu.VMEM((ng, SG, 1, LANES), jnp.int32),
                pltpu.VMEM((ng, NG + SPAD, 1, LANES), jnp.int32),
                pltpu.VMEM((ng, SG, 3, LANES), jnp.float32),
                pltpu.VMEM((ng, NG + SPAD, 3, LANES), jnp.float32),
                pltpu.VMEM((NG, 1, LANES), jnp.int32),
                pltpu.VMEM((NG, 3, LANES), jnp.float32),
                pltpu.VMEM((nw, VG, 4, LANES), jnp.float32),
                pltpu.VMEM((nw, NG + VPAD, 4, LANES), jnp.float32),
                dma((8,)),
                dma((ng,)), dma((ng,)), dma((nw,)), dma((nw,)),
                dma((ng,)), dma((ng,)), dma((ng,)), dma((ng,)),
                dma((nw,)), dma((nw,)), dma((nw,)), dma((nw,)),
                *[pltpu.VMEM((NG, 1, LANES), jnp.int32)] * nw,
            ],
            compiler_params=pltpu.CompilerParams(collective_id=0, has_side_effects=True),
        )(sbox, vbox, order, sbox, vbox, sdepth, scolor, vcolor, valpha, rentry, rstep)
        return frame[None, None]

    return jax.shard_map(
        per_device,
        mesh=mesh,
        in_specs=(
            P("wide", "grp", None, None),
            P("wide", "grp", None, None, None),
            P("wide", "grp", None, None),
            P("wide", "grp", None, None, None, None),
            P("wide", "grp", None, None, None),
            P("wide", "grp", None, None),
            P("wide", "grp", None, None),
            P("wide", "grp", None, None),
            P("grp", None),
        ),
        out_specs=P("grp", "wide", None, None),
        check_vma=False,
    )
```

```python
import functools

import jax
import jax.numpy as jnp
from jax import lax
from jax.experimental import pallas as pl
from jax.experimental.pallas import tpu as pltpu
from jax.sharding import PartitionSpec as P

TILE_H = 64
TILE_W = 64
SBOX_ROWS = 16
VBOX_ROWS = 32
LANES = 128

far_depth = 1073741824
MESH_ID = pl.DeviceIdType.MESH

NG = TILE_H * TILE_W // LANES
SG = SBOX_ROWS * TILE_W // LANES + 1
VG = VBOX_ROWS * TILE_W // LANES + 1
SPAD = NG - SG
VPAD = NG - VG


def group_of(top, pad):
    return jnp.minimum(lax.div(top * TILE_W, LANES), pad)


def window_inside(box, row, group, groups):
    top, bottom, left, right = [box(row, i) for i in range(4)]
    shape = (groups, 1, LANES)
    lane = lax.broadcasted_iota(jnp.int32, shape, 2)
    pix = lane + (lax.broadcasted_iota(jnp.int32, shape, 0) + group) * LANES
    col = lane & (TILE_W - 1)
    inside = (pix >= top * TILE_W) & (pix < bottom * TILE_W)
    return inside & (col >= left) & (col < right)


def groups_of(load, start, count):
    return jnp.stack([load(start + j) for j in range(count)])


def kernel(
    nw, ng, sbox_h, vbox_h, order_h, sdepth, scolor, vcolor, valpha, rentry, rstep,
    out,
    depth_in, scolor_in, color_in, alpha_in, entry_in, step_in,
    sbox_t, vbox, order, sbox_v, vbox_v, box_sem, sbox_r, vbox_r, sbox_m, vbox_m, dsend, drecv, csend, crecv, winner, surface, vsend, vrecv,
    load_sem, sb_s, sb_r, vb_s, vb_r, d_s, d_r, c_s, c_r, l_s, l_r, v_s, v_r, *limits,
):
    w = lax.axis_index("wide")
    g = lax.axis_index("grp")
    samples = alpha_in.shape[2]

    def sbox(r, i):
        return sbox_t[i, r]

    def vbox_at(c, i):
        return vbox[c, i]

    loads = [
        pltpu.make_async_copy(src, dst, load_sem.at[i])
        for i, (src, dst) in enumerate(
            [(sdepth, depth_in), (scolor, scolor_in), (valpha, alpha_in), (rentry, entry_in), (rstep, step_in), (vcolor, color_in)]
        )
    ]
    smalls = [
        pltpu.make_async_copy(src, dst, box_sem.at[i])
        for i, (src, dst) in enumerate(
            [(sbox_h, sbox_t), (sbox_h, sbox_v), (vbox_h, vbox_v), (vbox_h, vbox), (order_h, order)]
        )
    ]

    barrier = pltpu.get_barrier_semaphore()
    for i in range(1, ng):
        pl.semaphore_signal(barrier, inc=1, device_id=(w, lax.rem(g + i, ng)), device_id_type=MESH_ID)
    for i in range(1, nw):
        pl.semaphore_signal(barrier, inc=1, device_id=(lax.rem(w + i, nw), g), device_id_type=MESH_ID)
    loads[0].start()
    for copy in smalls:
        copy.start()
    for copy in loads[1:]:
        copy.start()

    smalls[0].wait()
    loads[0].wait()
    for r in range(ng):
        start = group_of(sbox(r, 0), SPAD)
        inside = window_inside(sbox, r, start, SG)
        depth = groups_of(lambda j: depth_in[j, r : r + 1], start, SG)
        dsend[r] = jnp.where(inside, depth, far_depth)

    for copy in smalls[1:]:
        copy.wait()
    pl.semaphore_wait(barrier, ng - 1 + nw - 1)

    def remote(src, dst, send, recv, device):
        return pltpu.make_async_remote_copy(
            src_ref=src, dst_ref=dst, send_sem=send, recv_sem=recv, device_id=device, device_id_type=MESH_ID
        )

    sends = []
    dcopies, ccopies, scopies, vbcopies = [], [], [], []
    for i in range(1, ng):
        peer = lax.rem(g + i, ng)
        scopies.append(remote(sbox_v, sbox_r.at[g], sb_s.at[i], sb_r.at[i], (w, peer)))
        scopies[-1].start()
    for i in range(1, ng):
        peer = lax.rem(g + i, ng)
        dcopies.append(
            remote(
                dsend.at[peer], drecv.at[g, pl.ds(SPAD, SG)], d_s.at[i], d_r.at[i], (w, peer)
            )
        )
        dcopies[-1].start()
    for i in range(1, nw):
        peer = lax.rem(w + i, nw)
        vbcopies.append(remote(vbox_v, vbox_r.at[w], vb_s.at[i], vb_r.at[i], (peer, g)))
        vbcopies[-1].start()
    loads[1].wait()
    for r in range(ng):
        start = group_of(sbox(r, 0), SPAD)
        for ch in range(3):
            color = groups_of(lambda j: scolor_in[ch, j].astype(jnp.float32)[r : r + 1], start, SG)
            csend[r, :, ch : ch + 1] = color
    middle = pl.ds(SPAD, SG)
    for i in range(1, ng):
        peer = lax.rem(g + i, ng)
        ccopies.append(remote(csend.at[peer], crecv.at[g, middle], c_s.at[i], c_r.at[i], (w, peer)))
        ccopies[-1].start()
    crecv[g, middle] = csend[g]

    sbox_r[g] = sbox_v[...]
    vbox_r[w] = vbox_v[...]
    drecv[g, middle] = dsend[g]
    for s in range(ng):
        drecv[s, :SPAD] = jnp.full((SPAD, 1, LANES), far_depth, jnp.int32)
        drecv[s, SPAD + SG :] = jnp.full((SPAD, 1, LANES), far_depth, jnp.int32)
    pad_row = lax.broadcasted_iota(jnp.int32, (VPAD, 4, LANES), 1)
    pad = jnp.where(pad_row == 3, 1.0, 0.0)
    for b in range(nw):
        vrecv[b, :VPAD] = pad
        vrecv[b, VPAD + VG :] = pad

    for copy in scopies:
        copy.wait_recv()
    to_smem = pltpu.make_async_copy(sbox_r, sbox_m, load_sem.at[6])
    to_smem.start()
    to_smem.wait()
    starts = [SPAD - group_of(sbox_m[s, 0, g], SPAD) for s in range(ng)]
    for copy in dcopies:
        copy.wait_recv()
    step = NG // 4

    for q in range(4):
        best = groups_of(lambda j: drecv[0, j], starts[0] + q * step, step)
        win = jnp.zeros_like(best)
        for s in range(1, ng):
            depth = groups_of(lambda j: drecv[s, j], starts[s] + q * step, step)
            win = jnp.where(depth < best, s, win)
            best = jnp.minimum(depth, best)
        limits[0][q * step : (q + 1) * step] = best
        winner[q * step : (q + 1) * step] = jnp.where(best < far_depth, win, -1)

    lcopies = []
    for i in range(1, nw):
        lcopies.append(remote(limits[0], limits[i], l_s.at[i], l_r.at[i], (lax.rem(w + i, nw), g)))
        lcopies[-1].start()
    for copy in loads[2:]:
        copy.wait()

    k_ids = lax.broadcasted_iota(jnp.int32, (VG, samples, LANES), 1)

    def integrate(c, limit):
        start = group_of(vbox[c, 0], VPAD)
        inside = window_inside(vbox_at, c, start, VG)
        bound = jnp.where(inside, groups_of(lambda j: limit[j], start, VG), -1)
        entry = groups_of(lambda j: entry_in[j, pl.ds(c, 1)], start, VG)
        stride = groups_of(lambda j: step_in[j, pl.ds(c, 1)], start, VG)
        kept = entry + k_ids * stride < bound
        alpha = groups_of(lambda j: alpha_in[c, j].astype(jnp.float32), start, VG)
        opacity = jnp.where(kept, alpha, 0.0)
        clear = 1.0 - opacity
        before = jnp.where(k_ids >= 1, pltpu.roll(clear, 1, 1), 1.0)
        shift = 1
        while shift < samples:
            before = before * jnp.where(k_ids >= shift, pltpu.roll(before, shift, 1), 1.0)
            shift *= 2
        weight = opacity * before
        accum = []
        for ch in range(3):
            color = groups_of(lambda j: color_in[c, ch, j].astype(jnp.float32), start, VG)
            accum.append(jnp.sum(weight * color, axis=1, keepdims=True))
        return accum, (before * clear)[:, samples - 1 : samples]

    accum, trans = integrate(w, limits[0])
    window = pl.ds(VPAD, VG)
    for ch in range(3):
        vrecv[w, window, ch : ch + 1] = accum[ch]
    vrecv[w, window, 3:4] = trans

    def vcopy(i):
        c = lax.rem(w + nw - i, nw)
        return remote(vsend.at[c], vrecv.at[w, window], v_s.at[i], v_r.at[i], (c, g))

    for i in range(1, nw):
        c = lax.rem(w + nw - i, nw)
        lcopies[i - 1].wait_recv()
        accum, trans = integrate(c, limits[i])
        for ch in range(3):
            vsend[c, :, ch : ch + 1] = accum[ch]
        vsend[c, :, 3:4] = trans
        vcopy(i).start()

    for copy in ccopies:
        copy.wait_recv()
    for q in range(4):
        win = winner[q * step : (q + 1) * step]
        color = jnp.zeros((step, 3, LANES), jnp.float32)
        for s in range(ng):
            color = jnp.where(win == s, groups_of(lambda j: crecv[s, j], starts[s] + q * step, step), color)
        surface[q * step : (q + 1) * step] = color

    for copy in vbcopies:
        copy.wait_recv()
    to_smem = pltpu.make_async_copy(vbox_r, vbox_m, load_sem.at[7])
    to_smem.start()
    to_smem.wait()
    ranks = [order[0, j] for j in range(nw)]
    offsets = [VPAD - group_of(vbox_m[b, w, 0], VPAD) for b in ranks]
    for i in range(1, nw):
        vcopy(i).wait_recv()
    for q in range(4):
        color = jnp.zeros((step, 3, LANES), jnp.float32)
        through = jnp.ones((step, 1, LANES), jnp.float32)
        for j in range(nw):
            layer = groups_of(lambda i: vrecv[ranks[j], i], offsets[j] + q * step, step)
            color = color + through * layer[:, 0:3]
            through = through * layer[:, 3:4]
        color = color + through * surface[q * step : (q + 1) * step]
        for j in range(step):
            at = slice((q * step + j) * LANES, (q * step + j + 1) * LANES)
            out[0:3, at] = color[j]
            out[3:4, at] = through[j]

    for copy in scopies + dcopies + vbcopies + ccopies + lcopies:
        copy.wait_send()
    for i in range(1, nw):
        vcopy(i).wait_send()


def solution(mesh):
    nw, ng = mesh.shape["wide"], mesh.shape["grp"]

    def per_device(sdepth, scolor, sbox, vcolor, valpha, vbox, rentry, rstep, order):
        sdepth, scolor, sbox = sdepth[0, 0], scolor[0, 0].transpose(1, 0, 2), sbox[0, 0].T
        vcolor, valpha, vbox = vcolor[0, 0].transpose(0, 2, 1, 3), valpha[0, 0], vbox[0, 0]
        rentry, rstep = rentry[0, 0], rstep[0, 0]
        pix = TILE_H * TILE_W

        def grouped(x):
            x = x.reshape(x.shape[:-1] + (NG, LANES))
            return jnp.moveaxis(x, -2, -3)

        sdepth, scolor, vcolor, valpha = grouped(sdepth), grouped(scolor), grouped(vcolor), grouped(valpha)
        rentry, rstep = grouped(rentry), grouped(rstep)
        vmem = pl.BlockSpec(memory_space=pltpu.VMEM)
        hbm = pl.BlockSpec(memory_space=pl.ANY)
        dma = pltpu.SemaphoreType.DMA
        frame = pl.pallas_call(
            functools.partial(kernel, nw, ng),
            out_shape=jax.ShapeDtypeStruct((4, pix), jnp.float32),
            in_specs=[hbm] * 9,
            out_specs=vmem,
            scratch_shapes=[
                pltpu.VMEM(sdepth.shape, jnp.int32),
                pltpu.VMEM(scolor.shape, jnp.bfloat16),
                pltpu.VMEM(vcolor.shape, jnp.bfloat16),
                pltpu.VMEM(valpha.shape, jnp.bfloat16),
                pltpu.VMEM(rentry.shape, jnp.int32),
                pltpu.VMEM(rstep.shape, jnp.int32),
                pltpu.SMEM(sbox.shape, jnp.int32),
                pltpu.SMEM(vbox.shape, jnp.int32),
                pltpu.SMEM(order.shape, jnp.int32),
                pltpu.VMEM(sbox.shape, jnp.int32),
                pltpu.VMEM(vbox.shape, jnp.int32),
                dma((5,)),
                pltpu.VMEM((ng,) + sbox.shape, jnp.int32),
                pltpu.VMEM((nw,) + vbox.shape, jnp.int32),
                pltpu.SMEM((ng,) + sbox.shape, jnp.int32),
                pltpu.SMEM((nw,) + vbox.shape, jnp.int32),
                pltpu.VMEM((ng, SG, 1, LANES), jnp.int32),
                pltpu.VMEM((ng, NG + SPAD, 1, LANES), jnp.int32),
                pltpu.VMEM((ng, SG, 3, LANES), jnp.float32),
                pltpu.VMEM((ng, NG + SPAD, 3, LANES), jnp.float32),
                pltpu.VMEM((NG, 1, LANES), jnp.int32),
                pltpu.VMEM((NG, 3, LANES), jnp.float32),
                pltpu.VMEM((nw, VG, 4, LANES), jnp.float32),
                pltpu.VMEM((nw, NG + VPAD, 4, LANES), jnp.float32),
                dma((8,)),
                dma((ng,)), dma((ng,)), dma((nw,)), dma((nw,)),
                dma((ng,)), dma((ng,)), dma((ng,)), dma((ng,)),
                dma((nw,)), dma((nw,)), dma((nw,)), dma((nw,)),
                *[pltpu.VMEM((NG, 1, LANES), jnp.int32)] * nw,
            ],
            compiler_params=pltpu.CompilerParams(collective_id=0, has_side_effects=True),
        )(sbox, vbox, order, sdepth, scolor, vcolor, valpha, rentry, rstep)
        return frame[None, None]

    return jax.shard_map(
        per_device,
        mesh=mesh,
        in_specs=(
            P("wide", "grp", None, None),
            P("wide", "grp", None, None, None),
            P("wide", "grp", None, None),
            P("wide", "grp", None, None, None, None),
            P("wide", "grp", None, None, None),
            P("wide", "grp", None, None),
            P("wide", "grp", None, None),
            P("wide", "grp", None, None),
            P("grp", None),
        ),
        out_specs=P("grp", "wide", None, None),
        check_vma=False,
    )
```

```python
import functools

import jax
import jax.numpy as jnp
from jax import lax
from jax.experimental import pallas as pl
from jax.experimental.pallas import tpu as pltpu
from jax.sharding import PartitionSpec as P

TILE_H = 64
TILE_W = 64
SBOX_ROWS = 16
VBOX_ROWS = 32
LANES = 128

far_depth = 1073741824
ALPHA_MAX = 0.039794922
COLOR_MAX = 4.0
HALF = 32767.0
MESH_ID = pl.DeviceIdType.MESH

NG = TILE_H * TILE_W // LANES
SG = SBOX_ROWS * TILE_W // LANES + 1
VG = VBOX_ROWS * TILE_W // LANES + 1
SPAD = NG - SG
VPAD = NG - VG


def group_of(top, pad):
    return jnp.minimum(lax.div(top * TILE_W, LANES), pad)


def window_inside(box, row, group, groups):
    top, bottom, left, right = [box(row, i) for i in range(4)]
    shape = (groups, 1, LANES)
    lane = lax.broadcasted_iota(jnp.int32, shape, 2)
    pix = lane + (lax.broadcasted_iota(jnp.int32, shape, 0) + group) * LANES
    col = lane & (TILE_W - 1)
    inside = (pix >= top * TILE_W) & (pix < bottom * TILE_W)
    return inside & (col >= left) & (col < right)


def groups_of(load, start, count):
    return jnp.stack([load(start + j) for j in range(count)])


def kernel(
    nw, ng, sbox_h, vbox_h, order_h, sdepth, scolor, vcolor, valpha, rentry, rstep,
    out,
    depth_in, scolor_in, color_in, alpha_in, entry_in, step_in,
    sbox_t, vbox, order, sbox_v, vbox_v, box_sem, sbox_r, vbox_r, sbox_m, vbox_m, dsend, drecv, csend, crecv, winner, surface, seg, vsend, vrecv,
    load_sem, sb_s, sb_r, vb_s, vb_r, d_s, d_r, c_s, c_r, l_s, l_r, v_s, v_r, *limits,
):
    w = lax.axis_index("wide")
    g = lax.axis_index("grp")
    samples = alpha_in.shape[2]

    def sbox(r, i):
        return sbox_t[i, r]

    def vbox_at(c, i):
        return vbox[c, i]

    loads = [
        pltpu.make_async_copy(src, dst, load_sem.at[i])
        for i, (src, dst) in enumerate(
            [(sdepth, depth_in), (scolor, scolor_in), (valpha, alpha_in), (rentry, entry_in), (rstep, step_in), (vcolor, color_in)]
        )
    ]
    smalls = [
        pltpu.make_async_copy(src, dst, box_sem.at[i])
        for i, (src, dst) in enumerate(
            [(sbox_h, sbox_t), (sbox_h, sbox_v), (vbox_h, vbox_v), (vbox_h, vbox), (order_h, order)]
        )
    ]

    barrier = pltpu.get_barrier_semaphore()
    for i in range(1, ng):
        pl.semaphore_signal(barrier, inc=1, device_id=(w, lax.rem(g + i, ng)), device_id_type=MESH_ID)
    for i in range(1, nw):
        pl.semaphore_signal(barrier, inc=1, device_id=(lax.rem(w + i, nw), g), device_id_type=MESH_ID)
    loads[0].start()
    for copy in smalls:
        copy.start()
    for copy in loads[1:]:
        copy.start()

    smalls[0].wait()
    loads[0].wait()
    for r in range(ng):
        start = group_of(sbox(r, 0), SPAD)
        inside = window_inside(sbox, r, start, SG)
        depth = groups_of(lambda j: depth_in[j, r : r + 1], start, SG)
        dsend[r] = jnp.where(inside, depth, far_depth)

    for copy in smalls[1:]:
        copy.wait()
    pl.semaphore_wait(barrier, ng - 1 + nw - 1)

    def remote(src, dst, send, recv, device):
        return pltpu.make_async_remote_copy(
            src_ref=src, dst_ref=dst, send_sem=send, recv_sem=recv, device_id=device, device_id_type=MESH_ID
        )

    sends = []
    dcopies, ccopies, scopies, vbcopies = [], [], [], []
    for i in range(1, ng):
        peer = lax.rem(g + i, ng)
        scopies.append(remote(sbox_v, sbox_r.at[g], sb_s.at[i], sb_r.at[i], (w, peer)))
        scopies[-1].start()
    for i in range(1, ng):
        peer = lax.rem(g + i, ng)
        dcopies.append(
            remote(
                dsend.at[peer], drecv.at[g, pl.ds(SPAD, SG)], d_s.at[i], d_r.at[i], (w, peer)
            )
        )
        dcopies[-1].start()
    for i in range(1, nw):
        peer = lax.rem(w + i, nw)
        vbcopies.append(remote(vbox_v, vbox_r.at[w], vb_s.at[i], vb_r.at[i], (peer, g)))
        vbcopies[-1].start()
    loads[1].wait()
    for r in range(ng):
        start = group_of(sbox(r, 0), SPAD)
        for ch in range(3):
            color = groups_of(lambda j: scolor_in[ch, j].astype(jnp.float32)[r : r + 1], start, SG)
            csend[r, :, ch : ch + 1] = color
    middle = pl.ds(SPAD, SG)
    for i in range(1, ng):
        peer = lax.rem(g + i, ng)
        ccopies.append(remote(csend.at[peer], crecv.at[g, middle], c_s.at[i], c_r.at[i], (w, peer)))
        ccopies[-1].start()
    crecv[g, middle] = csend[g]

    sbox_r[g] = sbox_v[...]
    vbox_r[w] = vbox_v[...]
    drecv[g, middle] = dsend[g]
    for s in range(ng):
        drecv[s, :SPAD] = jnp.full((SPAD, 1, LANES), far_depth, jnp.int32)
        drecv[s, SPAD + SG :] = jnp.full((SPAD, 1, LANES), far_depth, jnp.int32)
    most = 1.001 * (1.0 - (1.0 - ALPHA_MAX) ** samples)
    pad = jnp.full((VPAD, 4, LANES), -HALF, jnp.float32).astype(jnp.int32).astype(jnp.int16)
    for b in range(nw):
        vrecv[b, :VPAD] = pad
        vrecv[b, VPAD + VG :] = pad

    for copy in scopies:
        copy.wait_recv()
    to_smem = pltpu.make_async_copy(sbox_r, sbox_m, load_sem.at[6])
    to_smem.start()
    to_smem.wait()
    starts = [SPAD - group_of(sbox_m[s, 0, g], SPAD) for s in range(ng)]
    for copy in dcopies:
        copy.wait_recv()
    step = NG // 4

    for q in range(4):
        best = groups_of(lambda j: drecv[0, j], starts[0] + q * step, step)
        win = jnp.zeros_like(best)
        for s in range(1, ng):
            depth = groups_of(lambda j: drecv[s, j], starts[s] + q * step, step)
            win = jnp.where(depth < best, s, win)
            best = jnp.minimum(depth, best)
        limits[0][q * step : (q + 1) * step] = best
        winner[q * step : (q + 1) * step] = jnp.where(best < far_depth, win, -1)

    lcopies = []
    for i in range(1, nw):
        lcopies.append(remote(limits[0], limits[i], l_s.at[i], l_r.at[i], (lax.rem(w + i, nw), g)))
        lcopies[-1].start()
    for copy in loads[2:]:
        copy.wait()

    k_ids = lax.broadcasted_iota(jnp.int32, (VG, samples, LANES), 1)

    def integrate(c, limit):
        start = group_of(vbox[c, 0], VPAD)
        inside = window_inside(vbox_at, c, start, VG)
        bound = jnp.where(inside, groups_of(lambda j: limit[j], start, VG), -1)
        entry = groups_of(lambda j: entry_in[j, pl.ds(c, 1)], start, VG)
        stride = groups_of(lambda j: step_in[j, pl.ds(c, 1)], start, VG)
        kept = entry + k_ids * stride < bound
        alpha = groups_of(lambda j: alpha_in[c, j].astype(jnp.float32), start, VG)
        opacity = jnp.where(kept, alpha, 0.0)
        clear = 1.0 - opacity
        before = jnp.where(k_ids >= 1, pltpu.roll(clear, 1, 1), 1.0)
        shift = 1
        while shift < samples:
            before = before * jnp.where(k_ids >= shift, pltpu.roll(before, shift, 1), 1.0)
            shift *= 2
        weight = opacity * before
        accum = []
        for ch in range(3):
            color = groups_of(lambda j: color_in[c, ch, j].astype(jnp.float32), start, VG)
            accum.append(jnp.sum(weight * color, axis=1, keepdims=True))
        return accum, (before * clear)[:, samples - 1 : samples]

    accum, trans = integrate(w, limits[0])
    window = pl.ds(VPAD, VG)

    def coded(accum, trans):
        for ch in range(3):
            seg[:, ch : ch + 1] = accum[ch] * (2.0 * HALF / (most * COLOR_MAX)) - HALF
        seg[:, 3:4] = (1.0 - trans) * (2.0 * HALF / most) - HALF
        return jnp.round(seg[...]).astype(jnp.int32).astype(jnp.int16)

    vrecv[w, window] = coded(accum, trans)

    def vcopy(i):
        c = lax.rem(w + nw - i, nw)
        return remote(vsend.at[c], vrecv.at[w, window], v_s.at[i], v_r.at[i], (c, g))

    for i in sorted(range(1, nw), key=lambda i: abs(i - nw // 2)):
        c = lax.rem(w + nw - i, nw)
        lcopies[i - 1].wait_recv()
        accum, trans = integrate(c, limits[i])
        vsend[c] = coded(accum, trans)
        vcopy(i).start()

    for copy in ccopies:
        copy.wait_recv()
    for q in range(4):
        win = winner[q * step : (q + 1) * step]
        color = jnp.zeros((step, 3, LANES), jnp.float32)
        for s in range(ng):
            color = jnp.where(win == s, groups_of(lambda j: crecv[s, j], starts[s] + q * step, step), color)
        surface[q * step : (q + 1) * step] = color

    for copy in vbcopies:
        copy.wait_recv()
    to_smem = pltpu.make_async_copy(vbox_r, vbox_m, load_sem.at[7])
    to_smem.start()
    to_smem.wait()
    ranks = [order[0, j] for j in range(nw)]
    offsets = [VPAD - group_of(vbox_m[b, w, 0], VPAD) for b in ranks]
    for i in range(1, nw):
        vcopy(i).wait_recv()
    for q in range(4):
        color = jnp.zeros((step, 3, LANES), jnp.float32)
        through = jnp.ones((step, 1, LANES), jnp.float32)
        for j in range(nw):
            layer = groups_of(
                lambda i: vrecv[ranks[j], i].astype(jnp.int32).astype(jnp.float32), offsets[j] + q * step, step
            )
            layer = (layer + HALF) * (most / (2.0 * HALF))
            color = color + through * (layer[:, 0:3] * COLOR_MAX)
            through = through * (1.0 - layer[:, 3:4])
        color = color + through * surface[q * step : (q + 1) * step]
        for j in range(step):
            at = slice((q * step + j) * LANES, (q * step + j + 1) * LANES)
            out[0:3, at] = color[j]
            out[3:4, at] = through[j]

    for copy in scopies + dcopies + vbcopies + ccopies + lcopies:
        copy.wait_send()
    for i in range(1, nw):
        vcopy(i).wait_send()


def solution(mesh):
    nw, ng = mesh.shape["wide"], mesh.shape["grp"]

    def per_device(sdepth, scolor, sbox, vcolor, valpha, vbox, rentry, rstep, order):
        sdepth, scolor, sbox = sdepth[0, 0], scolor[0, 0].transpose(1, 0, 2), sbox[0, 0].T
        vcolor, valpha, vbox = vcolor[0, 0].transpose(0, 2, 1, 3), valpha[0, 0], vbox[0, 0]
        rentry, rstep = rentry[0, 0], rstep[0, 0]
        pix = TILE_H * TILE_W

        def grouped(x):
            x = x.reshape(x.shape[:-1] + (NG, LANES))
            return jnp.moveaxis(x, -2, -3)

        sdepth, scolor, vcolor, valpha = grouped(sdepth), grouped(scolor), grouped(vcolor), grouped(valpha)
        rentry, rstep = grouped(rentry), grouped(rstep)
        vmem = pl.BlockSpec(memory_space=pltpu.VMEM)
        hbm = pl.BlockSpec(memory_space=pl.ANY)
        dma = pltpu.SemaphoreType.DMA
        frame = pl.pallas_call(
            functools.partial(kernel, nw, ng),
            out_shape=jax.ShapeDtypeStruct((4, pix), jnp.float32),
            in_specs=[hbm] * 9,
            out_specs=vmem,
            scratch_shapes=[
                pltpu.VMEM(sdepth.shape, jnp.int32),
                pltpu.VMEM(scolor.shape, jnp.bfloat16),
                pltpu.VMEM(vcolor.shape, jnp.bfloat16),
                pltpu.VMEM(valpha.shape, jnp.bfloat16),
                pltpu.VMEM(rentry.shape, jnp.int32),
                pltpu.VMEM(rstep.shape, jnp.int32),
                pltpu.SMEM(sbox.shape, jnp.int32),
                pltpu.SMEM(vbox.shape, jnp.int32),
                pltpu.SMEM(order.shape, jnp.int32),
                pltpu.VMEM(sbox.shape, jnp.int32),
                pltpu.VMEM(vbox.shape, jnp.int32),
                dma((5,)),
                pltpu.VMEM((ng,) + sbox.shape, jnp.int32),
                pltpu.VMEM((nw,) + vbox.shape, jnp.int32),
                pltpu.SMEM((ng,) + sbox.shape, jnp.int32),
                pltpu.SMEM((nw,) + vbox.shape, jnp.int32),
                pltpu.VMEM((ng, SG, 1, LANES), jnp.int32),
                pltpu.VMEM((ng, NG + SPAD, 1, LANES), jnp.int32),
                pltpu.VMEM((ng, SG, 3, LANES), jnp.float32),
                pltpu.VMEM((ng, NG + SPAD, 3, LANES), jnp.float32),
                pltpu.VMEM((NG, 1, LANES), jnp.int32),
                pltpu.VMEM((NG, 3, LANES), jnp.float32),
                pltpu.VMEM((VG, 4, LANES), jnp.float32),
                pltpu.VMEM((nw, VG, 4, LANES), jnp.int16),
                pltpu.VMEM((nw, NG + VPAD, 4, LANES), jnp.int16),
                dma((8,)),
                dma((ng,)), dma((ng,)), dma((nw,)), dma((nw,)),
                dma((ng,)), dma((ng,)), dma((ng,)), dma((ng,)),
                dma((nw,)), dma((nw,)), dma((nw,)), dma((nw,)),
                *[pltpu.VMEM((NG, 1, LANES), jnp.int32)] * nw,
            ],
            compiler_params=pltpu.CompilerParams(collective_id=0, has_side_effects=True),
        )(sbox, vbox, order, sdepth, scolor, vcolor, valpha, rentry, rstep)
        return frame[None, None]

    return jax.shard_map(
        per_device,
        mesh=mesh,
        in_specs=(
            P("wide", "grp", None, None),
            P("wide", "grp", None, None, None),
            P("wide", "grp", None, None),
            P("wide", "grp", None, None, None, None),
            P("wide", "grp", None, None, None),
            P("wide", "grp", None, None),
            P("wide", "grp", None, None),
            P("wide", "grp", None, None),
            P("grp", None),
        ),
        out_specs=P("grp", "wide", None, None),
        check_vma=False,
    )
```
